32 devices in a mesh: freq: 8 (over z, x), tm: 4 (over y, core).
Axes of the slice: x: 2, y: 2, z: 4, core: 2. Of those that a mesh axis runs over, the one named last changes fastest.
Arguments:
- vis: bfloat16 [16, 8, 16, 2, 128, 128], P('freq', 'tm'), may hold values from -6 to 6
- model: bfloat16 [16, 8, 16, 2, 128, 128], P('freq', 'tm'), may hold values from -6 to 6
- block_rows: int32 [16, 8, 16], P('freq', 'tm'), may hold values from 0 to 15
- block_cols: int32 [16, 8, 16], P('freq', 'tm'), may hold values from 0 to 15
- flags: int32 [16, 8, 16], P('freq', 'tm'), may hold values 0 or 1
- prior: float32 [16, 8, 2, 2048], P('freq', 'tm'), may hold values from -6 to 6
- couplings: float32 [3, 2048], replicated, may hold values from 0.1 to 0.6
- damping: float32 [2048], replicated, may hold values from 8 to 128
Outputs:
- gains: float32 [16, 8, 2, 2048], P('freq', 'tm')
- changes: float32 [4], replicated
The draws below stay inside these ranges and needn't reach their ends.
All inputs are finite; a program needn't handle non-finite values. No bound on the sum of `flags` on one device may be relied on, other than what follows from the above.
Results may differ from the reference program's by a relative error of at most 0.0003.
Values sent between devices are 32-bit elements; how exact they have to be, the bound alone decides.
A program may use at most 64 MiB of HBM per device.

```python
import math
import jax
import jax.numpy as jnp
from jax import lax

N = 2048
BS = 128
NB = 16
BLK = 16
ITERS = 4
FREQ = 16
TIMES = 8


def place_ends(result, stream_key, low, top_value):
    index_at = [jax.random.randint(jax.random.fold_in(stream_key, axis), (), 0, length) for axis, length in enumerate(result.shape)]
    longest = result.shape.index(max(result.shape))
    neighbour = index_at[:longest] + [(index_at[longest] + 1) % result.shape[longest]] + index_at[longest + 1:]
    return result.at[tuple(index_at)].set(low).at[tuple(neighbour)].set(top_value)


def block_scale(stream_key, dims, pieces, least, top_value):
    def one(axis_at, shards_of):
        heights = jax.random.uniform(jax.random.fold_in(jax.random.fold_in(stream_key, 6), axis_at), (shards_of,), jnp.float32, least / len(pieces), top_value / len(pieces))
        return jnp.repeat(jnp.exp(heights), dims[axis_at] // shards_of).reshape((-1,) + (1,) * (len(dims) - axis_at - 1))

    level = one(*pieces[0])
    for cut in pieces[1:]:
        level = level * one(*cut)
    return level


def centred(key, dims, scale, reach, pieces=(), held_as=jnp.bfloat16):
    result = jax.random.normal(key, dims, jnp.float32) * scale
    if len(pieces) > 0:
        result = block_scale(key, dims, pieces, -0.22, 0.18) * result
    return jnp.clip(result, min=-reach, max=reach).astype(held_as)


def setup_inputs(seed: int = 0) -> dict:
    seeds = jax.random.split(jax.random.key(seed), 9)
    vis = centred(seeds[0], (FREQ, TIMES, BLK, 2, BS, BS), 1.0, 6.0, ((0, 8), (1, 4)))
    model = centred(seeds[1], (FREQ, TIMES, BLK, 2, BS, BS), 1.0, 6.0, ((0, 8), (1, 4)))
    block_rows = place_ends(jax.random.randint(seeds[2], (FREQ, TIMES, BLK), 0, NB), jax.random.fold_in(seeds[2], 1), 0, NB - 1).astype(jnp.int32)
    block_cols = place_ends(jax.random.randint(seeds[3], (FREQ, TIMES, BLK), 0, NB), jax.random.fold_in(seeds[3], 1), 0, NB - 1).astype(jnp.int32)
    flags = place_ends((jax.random.randint(seeds[4], (FREQ, TIMES, BLK), 0, 4) < 3).astype(jnp.int32), jax.random.fold_in(seeds[4], 1), 0, 1)
    prior = centred(seeds[5], (FREQ, TIMES, 2, N), 1.0, 6.0, ((0, 8), (1, 4)), jnp.float32)
    couplings = jnp.clip(jnp.exp(jax.random.uniform(seeds[6], (3, N), jnp.float32, math.log(0.1), math.log(0.6))), 0.1, 0.6)
    damping = jnp.clip(jnp.exp(jax.random.uniform(seeds[7], (N,), jnp.float32, math.log(8.0), math.log(128.0))), 8.0, 128.0)
    return {"vis": vis, "model": model, "block_rows": block_rows, "block_cols": block_cols, "flags": flags, "prior": prior, "couplings": couplings, "damping": damping}


def tile_terms(gains, rows, cols, flags, vis, model):
    width = vis.shape[-1]
    blocks = gains.shape[-1] // width
    count = gains.shape[0]
    gain_blocks = gains.reshape(count, 2, blocks, width)
    labels = jnp.arange(blocks, dtype=jnp.int32)
    row_hot = (rows[..., None] == labels).astype(jnp.float32)
    col_hot = (cols[..., None] == labels).astype(jnp.float32)
    row_gain = jnp.einsum('kbn,kcnr->kbcr', row_hot, gain_blocks, precision=lax.Precision.HIGHEST)
    grow_re = row_gain[:, :, 0][..., None]
    grow_im = row_gain[:, :, 1][..., None]
    model_re = model[:, :, 0].astype(jnp.float32)
    model_im = model[:, :, 1].astype(jnp.float32)
    vis_re = vis[:, :, 0].astype(jnp.float32)
    vis_im = vis[:, :, 1].astype(jnp.float32)
    zeta_re = grow_re * model_re - grow_im * model_im
    zeta_im = grow_re * model_im + grow_im * model_re
    num_re = lax.optimization_barrier(jnp.sum(vis_re * zeta_re + vis_im * zeta_im, axis=-2))
    num_im = lax.optimization_barrier(jnp.sum(vis_re * zeta_im - vis_im * zeta_re, axis=-2))
    denom = lax.optimization_barrier(jnp.sum(zeta_re * zeta_re + zeta_im * zeta_im, axis=-2))
    terms = jnp.stack([num_re, num_im, denom], axis=2) * flags.astype(jnp.float32)[..., None, None]
    summed = jnp.einsum('kbn,kbcr->kcnr', col_hot, terms, precision=lax.Precision.HIGHEST)
    return summed.reshape(count, 3, blocks * width)

def reference(vis, model, block_rows, block_cols, flags, prior, couplings, damping):
    prior_prev = jnp.roll(prior, 1, axis=0)
    current = prior
    changes = []
    for step in range(ITERS):
        terms = lax.map(lambda items: tile_terms(*items), (current, block_rows, block_cols, flags, vis, model))
        near = jnp.roll(terms, 1, axis=0) + jnp.roll(terms, -1, axis=0)
        far = jnp.roll(terms, 2, axis=0) + jnp.roll(terms, -2, axis=0)
        padded = jnp.pad(terms, ((0, 0), (1, 1), (0, 0), (0, 0)))
        later = padded[:, :-2] + padded[:, 2:]
        smooth = terms + couplings[0] * near + couplings[1] * far + couplings[2] * later
        numer = smooth[:, :, 0:2] + damping * prior_prev
        denom = smooth[:, :, 2] + damping
        fresh = numer / denom[:, :, None]
        if step % 2 == 1:
            fresh = 0.5 * (fresh + current)
        change = jnp.sum((fresh - current) ** 2)
        scale = jnp.sum(fresh * fresh)
        changes.append(jnp.sqrt(change / (scale + 1e-06)))
        current = fresh
    return (current, jnp.stack(changes))
```

```python
import functools

import jax
import jax.numpy as jnp
from jax import lax
from jax.experimental import pallas as pl
from jax.experimental.pallas import tpu as pltpu
from jax.sharding import PartitionSpec as P

ITERS = 4
REACH = 2
MESH = pl.DeviceIdType.MESH
F32 = jnp.float32
BF16 = jnp.bfloat16


def split(value):
    high = value.astype(BF16)
    return high, (value - high.astype(F32)).astype(BF16)


def kernel(
    dims,
    vis_ref, model_ref, rows_ref, cols_ref, flags_ref, prior_ref, coup_ref, damp_ref,
    gains_ref, changes_ref,
    vbuf, mbuf, wa, wb, gain, prev, coef, from_prior, terms, low, high, early, late,
    stats, all_freq, part, all_tm,
    load_sem, prior_sem, up_send, down_send, low_recv, high_recv,
    early_send, late_send, early_recv, late_recv, freq_send, freq_recv, tm_send, tm_recv,
):
    nf, nt, ftiles, ttiles, blks, width, nb = dims
    fi = lax.axis_index("freq")
    ti = lax.axis_index("tm")
    above, below = lax.rem(fi + 1, nf), lax.rem(fi + nf - 1, nf)
    tiles = [(f, t) for f in range(ftiles) for t in range(ttiles)]

    barrier = pltpu.get_barrier_semaphore()
    for step in range(1, nf):
        pl.semaphore_signal(
            barrier, inc=1, device_id={"freq": lax.rem(fi + step, nf)}, device_id_type=MESH
        )
    for step in range(1, nt):
        pl.semaphore_signal(
            barrier, inc=1, device_id={"tm": lax.rem(ti + step, nt)}, device_id_type=MESH
        )

    def loads(f, t):
        i = f * ttiles + t
        return (
            pltpu.make_async_copy(vis_ref.at[f, t], vbuf.at[i], load_sem.at[0, i]),
            pltpu.make_async_copy(model_ref.at[f, t], mbuf.at[i], load_sem.at[1, i]),
        )

    for f, t in tiles:
        for copy in loads(f, t):
            copy.start()

    for f, t in tiles:
        i = f * ttiles + t
        for c in range(2):
            for n in range(nb):
                gain[i, c, n : n + 1, :] = prior_ref[f, t, c : c + 1, n * width : (n + 1) * width]
    for n in range(nb):
        for c in range(3):
            coef[c, n : n + 1, :] = coup_ref[c : c + 1, n * width : (n + 1) * width]
        coef[3, n : n + 1, :] = damp_ref[0:1, n * width : (n + 1) * width]

    @pl.when(ti == 0)
    def _():
        early[...] = jnp.zeros_like(early)

    @pl.when(ti == nt - 1)
    def _():
        late[...] = jnp.zeros_like(late)

    pl.semaphore_wait(barrier, nf - 1 + nt - 1)

    prior_copy = pltpu.make_async_remote_copy(
        src_ref=prior_ref.at[ftiles - 1], dst_ref=from_prior,
        send_sem=prior_sem.at[0], recv_sem=prior_sem.at[1],
        device_id={"freq": above}, device_id_type=MESH,
    )
    prior_copy.start()

    def up_copy(k, f, t):
        s = (f - (ftiles - REACH)) * ttiles + t
        return pltpu.make_async_remote_copy(
            src_ref=terms.at[k, f * ttiles + t], dst_ref=low.at[k, s],
            send_sem=up_send.at[k, s], recv_sem=low_recv.at[k, s],
            device_id={"freq": above}, device_id_type=MESH,
        )

    def down_copy(k, f, t):
        s = f * ttiles + t
        return pltpu.make_async_remote_copy(
            src_ref=terms.at[k, f * ttiles + t], dst_ref=high.at[k, s],
            send_sem=down_send.at[k, s], recv_sem=high_recv.at[k, s],
            device_id={"freq": below}, device_id_type=MESH,
        )

    def later_copy(k, f):
        return pltpu.make_async_remote_copy(
            src_ref=terms.at[k, f * ttiles + ttiles - 1], dst_ref=early.at[k, f],
            send_sem=early_send.at[k, f], recv_sem=early_recv.at[k, f],
            device_id={"tm": jnp.minimum(ti + 1, nt - 1)}, device_id_type=MESH,
        )

    def earlier_copy(k, f):
        return pltpu.make_async_remote_copy(
            src_ref=terms.at[k, f * ttiles], dst_ref=late.at[k, f],
            send_sem=late_send.at[k, f], recv_sem=late_recv.at[k, f],
            device_id={"tm": jnp.maximum(ti - 1, 0)}, device_id_type=MESH,
        )

    def prepare(i):
        def one(b, carry):
            v_re = vbuf[i, b, 0].astype(F32)
            v_im = vbuf[i, b, 1].astype(F32)
            m_re = mbuf[i, b, 0].astype(F32)
            m_im = mbuf[i, b, 1].astype(F32)
            re_hi, re_lo = split(v_re * m_re + v_im * m_im)
            im_hi, im_lo = split(v_re * m_im - v_im * m_re)
            sq_hi, sq_lo = split(m_re * m_re + m_im * m_im)
            wa[i * blks + b, 0:width, 0:width] = re_hi
            wa[i * blks + b, width:, 0:width] = im_hi
            wa[i * blks + b, 0:width, width:] = sq_hi
            wa[i * blks + b, width:, width:] = sq_lo
            wb[i * blks + b, 0:width, :] = re_lo
            wb[i * blks + b, width:, :] = im_lo
            return carry

        lax.fori_loop(0, blks, one, 0)

    row_of = lax.broadcasted_iota(jnp.int32, (8, width), 0)
    block_of = lax.broadcasted_iota(jnp.int32, (nb, width), 0)

    def tile_terms(k, f, t):
        i = f * ttiles + t
        total = [jnp.zeros((nb, width), F32) for _ in range(3)]
        for b in range(blks):
            row = rows_ref[f, t, b]
            col = jnp.where(flags_ref[f, t, b] != 0, cols_ref[f, t, b], -1)
            re = jnp.broadcast_to(gain[i, 0, pl.ds(row, 1), :], (8, width))
            im = jnp.broadcast_to(gain[i, 1, pl.ds(row, 1), :], (8, width))
            sq = re * re + im * im
            left = jnp.where(row_of == 0, re, jnp.where(row_of == 1, im, sq))
            right = jnp.where(row_of == 0, -im, jnp.where(row_of == 1, re, sq))
            lhs = jnp.concatenate([left, right], axis=1)
            lhs_hi = lhs.astype(BF16).astype(F32)
            lhs = jnp.concatenate([lhs_hi, lhs - lhs_hi], axis=0).astype(BF16)
            out_a = jnp.dot(lhs, wa[i * blks + b], preferred_element_type=F32)
            out_b = jnp.dot(lhs, wb[i * blks + b], preferred_element_type=F32)
            out_a = out_a[0:8] + out_a[8:16]
            num = out_a[:, 0:width] + (out_b[0:8] + out_b[8:16])
            den = out_a[:, width:]
            hit = block_of == col
            parts = (num[0:1], num[1:2], den[2:3])
            total = [
                acc + jnp.where(hit, jnp.broadcast_to(one, (nb, width)), 0.0)
                for acc, one in zip(total, parts)
            ]
        for c in range(3):
            terms[k, i, c] = total[c]

    def iteration(k, carry):
        for f, t in tiles:
            i = f * ttiles + t

            @pl.when(k == 0)
            def _():
                for copy in loads(f, t):
                    copy.wait()
                prepare(i)

            tile_terms(k, f, t)
            if f >= ftiles - REACH:
                up_copy(k, f, t).start()
            if f < REACH:
                down_copy(k, f, t).start()
            if t == ttiles - 1:
                @pl.when(ti < nt - 1)
                def _():
                    later_copy(k, f).start()
            if t == 0:
                @pl.when(ti > 0)
                def _():
                    earlier_copy(k, f).start()

        @pl.when(k == 0)
        def _():
            prior_copy.wait_recv()
            for f, t in tiles:
                i = f * ttiles + t
                for c in range(2):
                    if f == 0:
                        for n in range(nb):
                            prev[i, c, n : n + 1, :] = from_prior[
                                t, c : c + 1, n * width : (n + 1) * width
                            ]
                        prev[i, c] = prev[i, c] * coef[3]
                    else:
                        prev[i, c] = gain[i - ttiles, c] * coef[3]

        for f in range(ftiles):
            @pl.when(ti > 0)
            def _():
                later_copy(k, f).wait_recv()

            @pl.when(ti < nt - 1)
            def _():
                earlier_copy(k, f).wait_recv()

        for f in range(ftiles - REACH, ftiles):
            for t in range(ttiles):
                up_copy(k, f, t).wait_recv()
        for f in range(REACH):
            for t in range(ttiles):
                down_copy(k, f, t).wait_recv()

        def at(f, t, c):
            if t < 0:
                return early[k, f, c]
            if t >= ttiles:
                return late[k, f, c]
            if f < 0:
                return low[k, (f + REACH) * ttiles + t, c]
            if f >= ftiles:
                return high[k, (f - ftiles) * ttiles + t, c]
            return terms[k, f * ttiles + t, c]

        odd = lax.rem(k, 2) == 1
        change = jnp.zeros((nb, width), F32)
        scale = jnp.zeros((nb, width), F32)
        for f, t in tiles:
            i = f * ttiles + t
            sums = [
                at(f, t, c)
                + coef[0] * (at(f - 1, t, c) + at(f + 1, t, c))
                + coef[1] * (at(f - 2, t, c) + at(f + 2, t, c))
                + coef[2] * (at(f, t - 1, c) + at(f, t + 1, c))
                for c in range(3)
            ]
            denom = sums[2] + coef[3]
            for c in range(2):
                old = gain[i, c]
                fresh = (sums[c] + prev[i, c]) / denom
                fresh = jnp.where(odd, 0.5 * (fresh + old), fresh)
                diff = fresh - old
                change = change + diff * diff
                scale = scale + fresh * fresh
                gain[i, c] = fresh
        stats[pl.ds(k, 1), :] = jnp.sum(change, axis=0, keepdims=True)
        stats[pl.ds(k + ITERS, 1), :] = jnp.sum(scale, axis=0, keepdims=True)
        return carry

    lax.fori_loop(0, ITERS, iteration, 0)

    def spread(axis, me, count, src, dst, send, recv):
        copies = [
            pltpu.make_async_remote_copy(
                src_ref=src, dst_ref=dst.at[me], send_sem=send.at[step], recv_sem=recv.at[me],
                device_id={axis: lax.rem(me + step, count)}, device_id_type=MESH,
            )
            for step in range(1, count)
        ]
        for copy in copies:
            copy.start()
        dst[me] = src[...]
        return copies

    def gathered(axis, me, count, src, dst, send, recv):
        for step in range(1, count):
            other = lax.rem(me + step, count)
            pltpu.make_async_remote_copy(
                src_ref=src, dst_ref=dst.at[other], send_sem=send.at[step],
                recv_sem=recv.at[other], device_id={axis: other}, device_id_type=MESH,
            ).wait_recv()
        return functools.reduce(lambda a, b: a + b, [dst[s] for s in range(count)])

    first = ("freq", fi, nf, stats, all_freq, freq_send, freq_recv)
    sent = spread(*first)
    for f, t in tiles:
        i = f * ttiles + t
        for c in range(2):
            for n in range(nb):
                gains_ref[f, t, c : c + 1, n * width : (n + 1) * width] = gain[i, c, n : n + 1, :]
    part[...] = gathered(*first)
    second = ("tm", ti, nt, part, all_tm, tm_send, tm_recv)
    sent += spread(*second)

    def drain(k, carry):
        for f, t in tiles:
            if f >= ftiles - REACH:
                up_copy(k, f, t).wait_send()
            if f < REACH:
                down_copy(k, f, t).wait_send()
        for f in range(ftiles):
            @pl.when(ti < nt - 1)
            def _():
                later_copy(k, f).wait_send()

            @pl.when(ti > 0)
            def _():
                earlier_copy(k, f).wait_send()
        return carry

    lax.fori_loop(0, ITERS, drain, 0)
    prior_copy.wait_send()
    whole = jnp.sum(gathered(*second), axis=1, keepdims=True)
    for copy in sent:
        copy.wait_send()
    ratio = jnp.sqrt(whole[0:ITERS] / (whole[ITERS : 2 * ITERS] + 1e-06))
    changes_ref[...] = jnp.broadcast_to(ratio, (ITERS, width))


def per_device(vis, model, block_rows, block_cols, flags, prior, couplings, damping):
    nf, nt = lax.axis_size("freq"), lax.axis_size("tm")
    ftiles, ttiles, blks = vis.shape[:3]
    width = vis.shape[-1]
    nb = prior.shape[-1] // width
    count = ftiles * ttiles
    dims = (nf, nt, ftiles, ttiles, blks, width, nb)
    vmem = pl.BlockSpec(memory_space=pltpu.VMEM)
    smem = pl.BlockSpec(memory_space=pltpu.SMEM)
    hbm = pl.BlockSpec(memory_space=pl.ANY)
    dma = pltpu.SemaphoreType.DMA
    halo = REACH * ttiles
    gains, changes = pl.pallas_call(
        functools.partial(kernel, dims),
        name="stefcal",
        out_shape=(
            jax.ShapeDtypeStruct(prior.shape, F32),
            jax.ShapeDtypeStruct((ITERS, width), F32),
        ),
        in_specs=[hbm, hbm, smem, smem, smem, vmem, vmem, vmem],
        out_specs=(vmem, vmem),
        scratch_shapes=[
            pltpu.VMEM((count,) + vis.shape[2:], BF16),
            pltpu.VMEM((count,) + vis.shape[2:], BF16),
            pltpu.VMEM((count * blks, 2 * width, 2 * width), BF16),
            pltpu.VMEM((count * blks, 2 * width, width), BF16),
            pltpu.VMEM((count, 2, nb, width), F32),
            pltpu.VMEM((count, 2, nb, width), F32),
            pltpu.VMEM((4, nb, width), F32),
            pltpu.VMEM(prior.shape[1:], F32),
            pltpu.VMEM((ITERS, count, 3, nb, width), F32),
            pltpu.VMEM((ITERS, halo, 3, nb, width), F32),
            pltpu.VMEM((ITERS, halo, 3, nb, width), F32),
            pltpu.VMEM((ITERS, ftiles, 3, nb, width), F32),
            pltpu.VMEM((ITERS, ftiles, 3, nb, width), F32),
            pltpu.VMEM((2 * ITERS, width), F32),
            pltpu.VMEM((nf, 2 * ITERS, width), F32),
            pltpu.VMEM((2 * ITERS, width), F32),
            pltpu.VMEM((nt, 2 * ITERS, width), F32),
            dma((2, count)),
            dma((2,)),
            dma((ITERS, halo)),
            dma((ITERS, halo)),
            dma((ITERS, halo)),
            dma((ITERS, halo)),
            dma((ITERS, ftiles)),
            dma((ITERS, ftiles)),
            dma((ITERS, ftiles)),
            dma((ITERS, ftiles)),
            dma((nf,)),
            dma((nf,)),
            dma((nt,)),
            dma((nt,)),
        ],
        compiler_params=pltpu.CompilerParams(
            collective_id=0, has_side_effects=True, vmem_limit_bytes=48 * 1024 * 1024
        ),
    )(vis, model, block_rows, block_cols, flags, prior, couplings, damping.reshape(1, -1))
    return gains, changes[:, 0]


def solution(mesh):
    placed = (
        P("freq", "tm", None, None, None, None),
        P("freq", "tm", None, None, None, None),
        P("freq", "tm", None),
        P("freq", "tm", None),
        P("freq", "tm", None),
        P("freq", "tm", None, None),
        P(),
        P(),
    )
    return jax.shard_map(
        per_device,
        mesh=mesh,
        in_specs=placed,
        out_specs=(P("freq", "tm", None, None), P()),
        check_vma=False,
    )
```

```python
import functools

import jax
import jax.numpy as jnp
from jax import lax
from jax.experimental import pallas as pl
from jax.experimental.pallas import tpu as pltpu
from jax.sharding import PartitionSpec as P

ITERS = 4
REACH = 2
MESH = pl.DeviceIdType.MESH
F32 = jnp.float32
BF16 = jnp.bfloat16


def split(value):
    high = value.astype(BF16)
    return high, (value - high.astype(F32)).astype(BF16)


def kernel(
    dims,
    vis_ref, model_ref, rows_in, cols_in, flags_in, prior_in, coup_in, damp_in,
    gains_ref, changes_ref,
    rows_ref, cols_ref, flags_ref, prior_ref, coup_ref, damp_ref,
    vbuf, mbuf, wa, wb, gain, prev, coef, from_prior, terms, low, high, early, late,
    stats, all_stats,
    small_sem, load_sem, prior_sem, up_send, down_send, low_recv, high_recv,
    early_send, late_send, early_recv, late_recv, stats_send, stats_recv,
):
    nf, nt, ftiles, ttiles, blks, width, nb = dims
    fi = lax.axis_index("freq")
    ti = lax.axis_index("tm")
    above, below = lax.rem(fi + 1, nf), lax.rem(fi + nf - 1, nf)
    tiles = [(f, t) for f in range(ftiles) for t in range(ttiles)]

    devices = nf * nt
    me = fi * nt + ti

    def peer(step):
        other = lax.rem(me + step, devices)
        return other, {"freq": other // nt, "tm": lax.rem(other, nt)}

    small = [
        pltpu.make_async_copy(src, dst, small_sem.at[n])
        for n, (src, dst) in enumerate((
            (prior_in, prior_ref), (coup_in, coup_ref), (damp_in, damp_ref),
            (rows_in, rows_ref), (cols_in, cols_ref), (flags_in, flags_ref),
        ))
    ]
    for copy in small:
        copy.start()

    def loads(f, t):
        i = f * ttiles + t
        return (
            pltpu.make_async_copy(vis_ref.at[f, t], vbuf.at[i], load_sem.at[0, i]),
            pltpu.make_async_copy(model_ref.at[f, t], mbuf.at[i], load_sem.at[1, i]),
        )

    for f, t in tiles:
        for copy in loads(f, t):
            copy.start()

    barrier = pltpu.get_barrier_semaphore()

    def greet(step, carry):
        pl.semaphore_signal(barrier, inc=1, device_id=peer(step)[1], device_id_type=MESH)
        return carry

    lax.fori_loop(1, devices, greet, 0)
    for copy in small:
        copy.wait()

    for f, t in tiles:
        i = f * ttiles + t
        for c in range(2):
            for n in range(nb):
                gain[i, c, n : n + 1, :] = prior_ref[f, t, c : c + 1, n * width : (n + 1) * width]
    for n in range(nb):
        for c in range(3):
            coef[c, n : n + 1, :] = coup_ref[c : c + 1, n * width : (n + 1) * width]
        coef[3, n : n + 1, :] = damp_ref[0:1, n * width : (n + 1) * width]

    prior_copy = pltpu.make_async_remote_copy(
        src_ref=prior_ref.at[ftiles - 1], dst_ref=from_prior,
        send_sem=prior_sem.at[0], recv_sem=prior_sem.at[1],
        device_id={"freq": above}, device_id_type=MESH,
    )

    def up_copy(k, f, t):
        s = (f - (ftiles - REACH)) * ttiles + t
        return pltpu.make_async_remote_copy(
            src_ref=terms.at[k, f * ttiles + t], dst_ref=low.at[k, s],
            send_sem=up_send.at[k, s], recv_sem=low_recv.at[k, s],
            device_id={"freq": above}, device_id_type=MESH,
        )

    def down_copy(k, f, t):
        s = f * ttiles + t
        return pltpu.make_async_remote_copy(
            src_ref=terms.at[k, f * ttiles + t], dst_ref=high.at[k, s],
            send_sem=down_send.at[k, s], recv_sem=high_recv.at[k, s],
            device_id={"freq": below}, device_id_type=MESH,
        )

    def later_copy(k, f):
        return pltpu.make_async_remote_copy(
            src_ref=terms.at[k, f * ttiles + ttiles - 1], dst_ref=early.at[k, f],
            send_sem=early_send.at[k, f], recv_sem=early_recv.at[k, f],
            device_id={"tm": lax.rem(ti + 1, nt)}, device_id_type=MESH,
        )

    def earlier_copy(k, f):
        return pltpu.make_async_remote_copy(
            src_ref=terms.at[k, f * ttiles], dst_ref=late.at[k, f],
            send_sem=late_send.at[k, f], recv_sem=late_recv.at[k, f],
            device_id={"tm": lax.rem(ti + nt - 1, nt)}, device_id_type=MESH,
        )

    def prepare(i):
        def pair(p, carry):
            for side in range(2):
                b = 2 * p + side
                lo = side * width
                v_re = vbuf[i, b, 0].astype(F32)
                v_im = vbuf[i, b, 1].astype(F32)
                m_re = mbuf[i, b, 0].astype(F32)
                m_im = mbuf[i, b, 1].astype(F32)
                re_hi, re_lo = split(v_re * m_re + v_im * m_im)
                im_hi, im_lo = split(v_re * m_im - v_im * m_re)
                sq_hi, sq_lo = split(m_re * m_re + m_im * m_im)
                wa[i * blks + b, 0:width, 0:width] = re_hi
                wa[i * blks + b, width:, 0:width] = im_hi
                wa[i * blks + b, 0:width, width:] = sq_hi
                wa[i * blks + b, width:, width:] = sq_lo
                wb[i * (blks // 2) + p, 0:width, lo : lo + width] = re_lo
                wb[i * (blks // 2) + p, width:, lo : lo + width] = im_lo
            return carry

        lax.fori_loop(0, blks // 2, pair, 0)

    row_of = lax.broadcasted_iota(jnp.int32, (8, width), 0)
    block_of = lax.broadcasted_iota(jnp.int32, (nb, width), 0)

    def tile_terms(k, f, t):
        i = f * ttiles + t
        total = [jnp.zeros((nb, width), F32) for _ in range(3)]
        for p in range(blks // 2):
            highs, outs, cols = [], [], []
            for b in (2 * p, 2 * p + 1):
                row = rows_ref[f, t, b]
                cols.append(jnp.where(flags_ref[f, t, b] != 0, cols_ref[f, t, b], -1))
                re = jnp.broadcast_to(gain[i, 0, pl.ds(row, 1), :], (8, width))
                im = jnp.broadcast_to(gain[i, 1, pl.ds(row, 1), :], (8, width))
                sq = re * re + im * im
                left = jnp.where(row_of == 0, re, jnp.where(row_of == 1, im, sq))
                right = jnp.where(row_of == 0, -im, jnp.where(row_of == 1, re, sq))
                lhs = jnp.concatenate([left, right], axis=1)
                lhs_hi = lhs.astype(BF16).astype(F32)
                highs.append(lhs_hi)
                lhs = jnp.concatenate([lhs_hi, lhs - lhs_hi], axis=0).astype(BF16)
                out = jnp.dot(lhs, wa[i * blks + b], preferred_element_type=F32)
                outs.append(out[0:8] + out[8:16])
            low_out = jnp.dot(
                jnp.concatenate(highs, axis=0).astype(BF16),
                wb[i * (blks // 2) + p],
                preferred_element_type=F32,
            )
            low_outs = (low_out[0:8, 0:width], low_out[8:16, width:])
            for out, low_out, col in zip(outs, low_outs, cols):
                num = out[:, 0:width] + low_out
                den = out[:, width:]
                hit = block_of == col
                parts = (num[0:1], num[1:2], den[2:3])
                total = [
                    acc + jnp.where(hit, jnp.broadcast_to(one, (nb, width)), 0.0)
                    for acc, one in zip(total, parts)
                ]
        for c in range(3):
            terms[k, i, c] = total[c]

    def iteration(k, first):
        for f, t in tiles:
            i = f * ttiles + t
            if first:
                for copy in loads(f, t):
                    copy.wait()
                prepare(i)
            tile_terms(k, f, t)
            if first and i == 0:
                pl.semaphore_wait(barrier, devices - 1)
                prior_copy.start()
            if f >= ftiles - REACH:
                up_copy(k, f, t).start()
            if f < REACH:
                down_copy(k, f, t).start()
            if t == ttiles - 1:
                later_copy(k, f).start()
            if t == 0:
                earlier_copy(k, f).start()

        if first:
            prior_copy.wait_recv()
            for f, t in tiles:
                i = f * ttiles + t
                for c in range(2):
                    if f == 0:
                        for n in range(nb):
                            prev[i, c, n : n + 1, :] = from_prior[
                                t, c : c + 1, n * width : (n + 1) * width
                            ]
                        prev[i, c] = prev[i, c] * coef[3]
                    else:
                        prev[i, c] = gain[i - ttiles, c] * coef[3]

        for f in range(ftiles):
            later_copy(k, f).wait_recv()
            earlier_copy(k, f).wait_recv()
        for f in range(ftiles - REACH, ftiles):
            for t in range(ttiles):
                up_copy(k, f, t).wait_recv()
        for f in range(REACH):
            for t in range(ttiles):
                down_copy(k, f, t).wait_recv()

        def at(f, t, c):
            if t < 0:
                return jnp.where(ti > 0, early[k, f, c], 0.0)
            if t >= ttiles:
                return jnp.where(ti < nt - 1, late[k, f, c], 0.0)
            if f < 0:
                return low[k, (f + REACH) * ttiles + t, c]
            if f >= ftiles:
                return high[k, (f - ftiles) * ttiles + t, c]
            return terms[k, f * ttiles + t, c]

        odd = lax.rem(k, 2) == 1
        change = jnp.zeros((nb, width), F32)
        scale = jnp.zeros((nb, width), F32)
        for f, t in tiles:
            i = f * ttiles + t
            sums = [
                at(f, t, c)
                + coef[0] * (at(f - 1, t, c) + at(f + 1, t, c))
                + coef[1] * (at(f - 2, t, c) + at(f + 2, t, c))
                + coef[2] * (at(f, t - 1, c) + at(f, t + 1, c))
                for c in range(3)
            ]
            denom = sums[2] + coef[3]
            for c in range(2):
                old = gain[i, c]
                fresh = (sums[c] + prev[i, c]) / denom
                fresh = jnp.where(odd, 0.5 * (fresh + old), fresh)
                diff = fresh - old
                change = change + diff * diff
                scale = scale + fresh * fresh
                gain[i, c] = fresh
        sums = [
            jnp.sum(jnp.sum(x, axis=0, keepdims=True), axis=1, keepdims=True)
            for x in (change, scale)
        ]
        stats[...] = jnp.where(lane_of == k, jnp.concatenate(sums, axis=0), stats[...])

    lane_of = lax.broadcasted_iota(jnp.int32, (2, width), 1)
    stats[...] = jnp.zeros_like(stats)
    iteration(0, True)

    def rest(k, carry):
        iteration(k, False)
        return carry

    lax.fori_loop(1, ITERS, rest, 0)

    def stats_copy(step, slot):
        return pltpu.make_async_remote_copy(
            src_ref=stats, dst_ref=all_stats.at[slot],
            send_sem=stats_send.at[step], recv_sem=stats_recv.at[slot],
            device_id=peer(step)[1], device_id_type=MESH,
        )

    def send_stats(step, carry):
        stats_copy(step, me).start()
        return carry

    lax.fori_loop(1, devices, send_stats, 0)
    all_stats[me] = stats[...]

    for f, t in tiles:
        i = f * ttiles + t
        for c in range(2):
            for n in range(nb):
                gains_ref[f, t, c : c + 1, n * width : (n + 1) * width] = gain[i, c, n : n + 1, :]

    def drain(k, carry):
        for f, t in tiles:
            if f >= ftiles - REACH:
                up_copy(k, f, t).wait_send()
            if f < REACH:
                down_copy(k, f, t).wait_send()
        for f in range(ftiles):
            later_copy(k, f).wait_send()
            earlier_copy(k, f).wait_send()
        return carry

    lax.fori_loop(0, ITERS, drain, 0)
    prior_copy.wait_send()

    def finish(step, carry):
        stats_copy(step, me).wait_send()
        stats_copy(step, peer(step)[0]).wait_recv()
        return carry

    lax.fori_loop(1, devices, finish, 0)
    whole = jnp.sum(all_stats[...], axis=0)
    changes_ref[...] = jnp.sqrt(whole[0:1] / (whole[1:2] + 1e-06))


def per_device(vis, model, block_rows, block_cols, flags, prior, couplings, damping):
    nf, nt = lax.axis_size("freq"), lax.axis_size("tm")
    ftiles, ttiles, blks = vis.shape[:3]
    width = vis.shape[-1]
    nb = prior.shape[-1] // width
    count = ftiles * ttiles
    dims = (nf, nt, ftiles, ttiles, blks, width, nb)
    vmem = pl.BlockSpec(memory_space=pltpu.VMEM)
    hbm = pl.BlockSpec(memory_space=pltpu.HBM)
    dma = pltpu.SemaphoreType.DMA
    halo = REACH * ttiles
    gains, changes = pl.pallas_call(
        functools.partial(kernel, dims),
        name="stefcal",
        out_shape=(
            jax.ShapeDtypeStruct(prior.shape, F32),
            jax.ShapeDtypeStruct((1, width), F32),
        ),
        in_specs=[hbm] * 8,
        out_specs=(vmem, vmem),
        scratch_shapes=[
            pltpu.SMEM(block_rows.shape, jnp.int32),
            pltpu.SMEM(block_rows.shape, jnp.int32),
            pltpu.SMEM(block_rows.shape, jnp.int32),
            pltpu.VMEM(prior.shape, F32),
            pltpu.VMEM(couplings.shape, F32),
            pltpu.VMEM((1, damping.shape[0]), F32),
            pltpu.VMEM((count,) + vis.shape[2:], BF16),
            pltpu.VMEM((count,) + vis.shape[2:], BF16),
            pltpu.VMEM((count * blks, 2 * width, 2 * width), BF16),
            pltpu.VMEM((count * blks // 2, 2 * width, 2 * width), BF16),
            pltpu.VMEM((count, 2, nb, width), F32),
            pltpu.VMEM((count, 2, nb, width), F32),
            pltpu.VMEM((4, nb, width), F32),
            pltpu.VMEM(prior.shape[1:], F32),
            pltpu.VMEM((ITERS, count, 3, nb, width), F32),
            pltpu.VMEM((ITERS, halo, 3, nb, width), F32),
            pltpu.VMEM((ITERS, halo, 3, nb, width), F32),
            pltpu.VMEM((ITERS, ftiles, 3, nb, width), F32),
            pltpu.VMEM((ITERS, ftiles, 3, nb, width), F32),
            pltpu.VMEM((2, width), F32),
            pltpu.VMEM((nf * nt, 2, width), F32),
            dma((6,)),
            dma((2, count)),
            dma((2,)),
            dma((ITERS, halo)),
            dma((ITERS, halo)),
            dma((ITERS, halo)),
            dma((ITERS, halo)),
            dma((ITERS, ftiles)),
            dma((ITERS, ftiles)),
            dma((ITERS, ftiles)),
            dma((ITERS, ftiles)),
            dma((nf * nt,)),
            dma((nf * nt,)),
        ],
        compiler_params=pltpu.CompilerParams(
            collective_id=0, has_side_effects=True, vmem_limit_bytes=48 * 1024 * 1024
        ),
    )(vis, model, block_rows, block_cols, flags, prior, couplings, damping.reshape(1, -1))
    return gains, changes[0, :ITERS]


def solution(mesh):
    placed = (
        P("freq", "tm", None, None, None, None),
        P("freq", "tm", None, None, None, None),
        P("freq", "tm", None),
        P("freq", "tm", None),
        P("freq", "tm", None),
        P("freq", "tm", None, None),
        P(),
        P(),
    )
    return jax.shard_map(
        per_device,
        mesh=mesh,
        in_specs=placed,
        out_specs=(P("freq", "tm", None, None), P()),
        check_vma=False,
    )
```

```python
import functools

import jax
import jax.numpy as jnp
from jax import lax
from jax.experimental import pallas as pl
from jax.experimental.pallas import tpu as pltpu
from jax.sharding import PartitionSpec as P

ITERS = 4
REACH = 2
MESH = pl.DeviceIdType.MESH
F32 = jnp.float32
BF16 = jnp.bfloat16


def split(value):
    high = value.astype(BF16)
    return high, (value - high.astype(F32)).astype(BF16)


def kernel(
    dims,
    vis_ref, model_ref, rows_in, cols_in, flags_in, prior_in, coup_in, damp_in,
    gains_ref, changes_ref,
    rows_ref, cols_ref, flags_ref, prior_ref, coup_ref, damp_ref,
    vbuf, mbuf, wa, wb, gain, prev, coef, from_prior, terms, low, high, early, late,
    stats, all_stats,
    small_sem, load_sem, prior_sem, up_send, down_send, low_recv, high_recv,
    early_send, late_send, early_recv, late_recv, stats_send, stats_recv,
):
    nf, nt, ftiles, ttiles, blks, width, nb = dims
    fi = lax.axis_index("freq")
    ti = lax.axis_index("tm")
    above, below = lax.rem(fi + 1, nf), lax.rem(fi + nf - 1, nf)
    tiles = [(f, t) for f in range(ftiles) for t in range(ttiles)]

    devices = nf * nt
    me = fi * nt + ti

    def peer(step):
        other = lax.rem(me + step, devices)
        return other, {"freq": other // nt, "tm": lax.rem(other, nt)}

    small = [
        pltpu.make_async_copy(src, dst, small_sem.at[n])
        for n, (src, dst) in enumerate((
            (prior_in, prior_ref), (coup_in, coup_ref), (damp_in, damp_ref),
            (rows_in, rows_ref), (cols_in, cols_ref), (flags_in, flags_ref),
        ))
    ]
    for copy in small:
        copy.start()

    def loads(f, t):
        i = f * ttiles + t
        return (
            pltpu.make_async_copy(vis_ref.at[f, t], vbuf.at[i], load_sem.at[0, i]),
            pltpu.make_async_copy(model_ref.at[f, t], mbuf.at[i], load_sem.at[1, i]),
        )

    for f, t in tiles:
        for copy in loads(f, t):
            copy.start()

    barrier = pltpu.get_barrier_semaphore()

    def greet(step, carry):
        pl.semaphore_signal(barrier, inc=1, device_id=peer(step)[1], device_id_type=MESH)
        return carry

    lax.fori_loop(1, devices, greet, 0)
    for copy in small:
        copy.wait()

    for f, t in tiles:
        i = f * ttiles + t
        for c in range(2):
            for n in range(nb):
                gain[i, c, n : n + 1, :] = prior_ref[f, t, c : c + 1, n * width : (n + 1) * width]
    for n in range(nb):
        for c in range(3):
            coef[c, n : n + 1, :] = coup_ref[c : c + 1, n * width : (n + 1) * width]
        coef[3, n : n + 1, :] = damp_ref[0:1, n * width : (n + 1) * width]

    prior_copy = pltpu.make_async_remote_copy(
        src_ref=prior_ref.at[ftiles - 1], dst_ref=from_prior,
        send_sem=prior_sem.at[0], recv_sem=prior_sem.at[1],
        device_id={"freq": above}, device_id_type=MESH,
    )

    def up_copy(k, f, t):
        s = (f - (ftiles - REACH)) * ttiles + t
        return pltpu.make_async_remote_copy(
            src_ref=terms.at[k, f * ttiles + t], dst_ref=low.at[k, s],
            send_sem=up_send.at[k, s], recv_sem=low_recv.at[k, s],
            device_id={"freq": above}, device_id_type=MESH,
        )

    def down_copy(k, f, t):
        s = f * ttiles + t
        return pltpu.make_async_remote_copy(
            src_ref=terms.at[k, f * ttiles + t], dst_ref=high.at[k, s],
            send_sem=down_send.at[k, s], recv_sem=high_recv.at[k, s],
            device_id={"freq": below}, device_id_type=MESH,
        )

    def later_copy(k, f):
        return pltpu.make_async_remote_copy(
            src_ref=terms.at[k, f * ttiles + ttiles - 1], dst_ref=early.at[k, f],
            send_sem=early_send.at[k, f], recv_sem=early_recv.at[k, f],
            device_id={"tm": lax.rem(ti + 1, nt)}, device_id_type=MESH,
        )

    def earlier_copy(k, f):
        return pltpu.make_async_remote_copy(
            src_ref=terms.at[k, f * ttiles], dst_ref=late.at[k, f],
            send_sem=late_send.at[k, f], recv_sem=late_recv.at[k, f],
            device_id={"tm": lax.rem(ti + nt - 1, nt)}, device_id_type=MESH,
        )

    def prepare(i):
        def pair(p, carry):
            for side in range(2):
                b = 2 * p + side
                lo = side * width
                v_re = vbuf[i, b, 0].astype(F32)
                v_im = vbuf[i, b, 1].astype(F32)
                m_re = mbuf[i, b, 0].astype(F32)
                m_im = mbuf[i, b, 1].astype(F32)
                re_hi, re_lo = split(v_re * m_re + v_im * m_im)
                im_hi, im_lo = split(v_re * m_im - v_im * m_re)
                sq_hi, sq_lo = split(m_re * m_re + m_im * m_im)
                wa[i * blks + b, 0:width, 0:width] = re_hi
                wa[i * blks + b, width:, 0:width] = im_hi
                wa[i * blks + b, 0:width, width:] = sq_hi
                wa[i * blks + b, width:, width:] = sq_lo
                wb[i * (blks // 2) + p, 0:width, lo : lo + width] = re_lo
                wb[i * (blks // 2) + p, width:, lo : lo + width] = im_lo
            return carry

        lax.fori_loop(0, blks // 2, pair, 0)

    row_of = lax.broadcasted_iota(jnp.int32, (8, width), 0)
    block_of = lax.broadcasted_iota(jnp.int32, (nb, width), 0)

    def tile_terms(k, f, t):
        i = f * ttiles + t
        total = [jnp.zeros((nb, width), F32) for _ in range(3)]
        for p in range(blks // 2):
            highs, outs, cols = [], [], []
            for b in (2 * p, 2 * p + 1):
                row = rows_ref[f, t, b]
                cols.append(jnp.where(flags_ref[f, t, b] != 0, cols_ref[f, t, b], -1))
                re = jnp.broadcast_to(gain[i, 0, pl.ds(row, 1), :], (8, width))
                im = jnp.broadcast_to(gain[i, 1, pl.ds(row, 1), :], (8, width))
                sq = re * re + im * im
                left = jnp.where(row_of == 0, re, jnp.where(row_of == 1, im, sq))
                right = jnp.where(row_of == 0, -im, jnp.where(row_of == 1, re, sq))
                lhs = jnp.concatenate([left, right], axis=1)
                lhs_hi = lhs.astype(BF16).astype(F32)
                highs.append(lhs_hi)
                lhs = jnp.concatenate([lhs_hi, lhs - lhs_hi], axis=0).astype(BF16)
                out = jnp.dot(lhs, wa[i * blks + b], preferred_element_type=F32)
                outs.append(out[0:8] + out[8:16])
            low_out = jnp.dot(
                jnp.concatenate(highs, axis=0).astype(BF16),
                wb[i * (blks // 2) + p],
                preferred_element_type=F32,
            )
            low_outs = (low_out[0:8, 0:width], low_out[8:16, width:])
            for out, low_out, col in zip(outs, low_outs, cols):
                num = out[:, 0:width] + low_out
                den = out[:, width:]
                hit = block_of == col
                parts = (num[0:1], num[1:2], den[2:3])
                total = [
                    acc + jnp.where(hit, jnp.broadcast_to(one, (nb, width)), 0.0)
                    for acc, one in zip(total, parts)
                ]
        for c in range(3):
            terms[k, i, c] = total[c]

    def iteration(k, first):
        for f, t in tiles:
            i = f * ttiles + t
            if first:
                for copy in loads(f, t):
                    copy.wait()
                prepare(i)
            tile_terms(k, f, t)
            if first and i == 0:
                pl.semaphore_wait(barrier, devices - 1)
                prior_copy.start()
            if f >= ftiles - REACH:
                up_copy(k, f, t).start()
            if f < REACH:
                down_copy(k, f, t).start()
            if t == ttiles - 1:
                later_copy(k, f).start()
            if t == 0:
                earlier_copy(k, f).start()

        if first:
            prior_copy.wait_recv()
            for f, t in tiles:
                i = f * ttiles + t
                for c in range(2):
                    if f == 0:
                        for n in range(nb):
                            prev[i, c, n : n + 1, :] = from_prior[
                                t, c : c + 1, n * width : (n + 1) * width
                            ]
                        prev[i, c] = prev[i, c] * coef[3]
                    else:
                        prev[i, c] = gain[i - ttiles, c] * coef[3]

        for f in range(ftiles):
            later_copy(k, f).wait_recv()
            earlier_copy(k, f).wait_recv()
        for f in range(ftiles - REACH, ftiles):
            for t in range(ttiles):
                up_copy(k, f, t).wait_recv()
        for f in range(REACH):
            for t in range(ttiles):
                down_copy(k, f, t).wait_recv()

        def at(f, t, c):
            if t < 0:
                return jnp.where(ti > 0, early[k, f, c], 0.0)
            if t >= ttiles:
                return jnp.where(ti < nt - 1, late[k, f, c], 0.0)
            if f < 0:
                return low[k, (f + REACH) * ttiles + t, c]
            if f >= ftiles:
                return high[k, (f - ftiles) * ttiles + t, c]
            return terms[k, f * ttiles + t, c]

        odd = lax.rem(k, 2) == 1
        change = jnp.zeros((nb, width), F32)
        scale = jnp.zeros((nb, width), F32)
        for f, t in tiles:
            i = f * ttiles + t
            sums = [
                at(f, t, c)
                + coef[0] * (at(f - 1, t, c) + at(f + 1, t, c))
                + coef[1] * (at(f - 2, t, c) + at(f + 2, t, c))
                + coef[2] * (at(f, t - 1, c) + at(f, t + 1, c))
                for c in range(3)
            ]
            denom = sums[2] + coef[3]
            for c in range(2):
                old = gain[i, c]
                fresh = (sums[c] + prev[i, c]) / denom
                fresh = jnp.where(odd, 0.5 * (fresh + old), fresh)
                diff = fresh - old
                change = change + diff * diff
                scale = scale + fresh * fresh
                gain[i, c] = fresh
        sums = [
            jnp.sum(jnp.sum(x, axis=0, keepdims=True), axis=1, keepdims=True)
            for x in (change, scale)
        ]
        stats[...] = jnp.where(lane_of == k, jnp.concatenate(sums, axis=0), stats[...])

    lane_of = lax.broadcasted_iota(jnp.int32, (2, width), 1)
    stats[...] = jnp.zeros_like(stats)
    iteration(0, True)

    def rest(k, carry):
        iteration(k, False)
        return carry

    lax.fori_loop(1, ITERS, rest, 0)

    def stats_copy(step, slot):
        return pltpu.make_async_remote_copy(
            src_ref=stats, dst_ref=all_stats.at[slot],
            send_sem=stats_send.at[step], recv_sem=stats_recv.at[slot],
            device_id=peer(step)[1], device_id_type=MESH,
        )

    def send_stats(step, carry):
        stats_copy(step, me).start()
        return carry

    lax.fori_loop(1, devices, send_stats, 0)
    all_stats[me] = stats[...]

    for f, t in tiles:
        i = f * ttiles + t
        for c in range(2):
            for n in range(nb):
                gains_ref[f, t, c : c + 1, n * width : (n + 1) * width] = gain[i, c, n : n + 1, :]

    def drain(k, carry):
        for f, t in tiles:
            if f >= ftiles - REACH:
                up_copy(k, f, t).wait_send()
            if f < REACH:
                down_copy(k, f, t).wait_send()
        for f in range(ftiles):
            later_copy(k, f).wait_send()
            earlier_copy(k, f).wait_send()
        return carry

    lax.fori_loop(0, ITERS, drain, 0)
    prior_copy.wait_send()

    def finish(step, carry):
        stats_copy(step, me).wait_send()
        stats_copy(step, peer(step)[0]).wait_recv()
        return carry

    lax.fori_loop(1, devices, finish, 0)
    whole = jnp.sum(all_stats[...], axis=0)
    changes_ref[...] = jnp.sqrt(whole[0:1] / (whole[1:2] + 1e-06))


def per_device(vis, model, block_rows, block_cols, flags, prior, couplings, damping):
    nf, nt = lax.axis_size("freq"), lax.axis_size("tm")
    ftiles, ttiles, blks = vis.shape[:3]
    width = vis.shape[-1]
    nb = prior.shape[-1] // width
    count = ftiles * ttiles
    dims = (nf, nt, ftiles, ttiles, blks, width, nb)
    vmem = pl.BlockSpec(memory_space=pltpu.VMEM)
    hbm = pl.BlockSpec(memory_space=pltpu.HBM)
    dma = pltpu.SemaphoreType.DMA
    halo = REACH * ttiles
    gains, changes = pl.pallas_call(
        functools.partial(kernel, dims),
        name="stefcal",
        out_shape=(
            jax.ShapeDtypeStruct(prior.shape, F32),
            jax.ShapeDtypeStruct((1, width), F32),
        ),
        in_specs=[hbm] * 8,
        out_specs=(vmem, vmem),
        scratch_shapes=[
            pltpu.SMEM(block_rows.shape, jnp.int32),
            pltpu.SMEM(block_rows.shape, jnp.int32),
            pltpu.SMEM(block_rows.shape, jnp.int32),
            pltpu.VMEM(prior.shape, F32),
            pltpu.VMEM(couplings.shape, F32),
            pltpu.VMEM((1, damping.shape[0]), F32),
            pltpu.VMEM((count,) + vis.shape[2:], BF16),
            pltpu.VMEM((count,) + vis.shape[2:], BF16),
            pltpu.VMEM((count * blks, 2 * width, 2 * width), BF16),
            pltpu.VMEM((count * blks // 2, 2 * width, 2 * width), BF16),
            pltpu.VMEM((count, 2, nb, width), F32),
            pltpu.VMEM((count, 2, nb, width), F32),
            pltpu.VMEM((4, nb, width), F32),
            pltpu.VMEM(prior.shape[1:], F32),
            pltpu.VMEM((ITERS, count, 3, nb, width), F32),
            pltpu.VMEM((ITERS, halo, 3, nb, width), F32),
            pltpu.VMEM((ITERS, halo, 3, nb, width), F32),
            pltpu.VMEM((ITERS, ftiles, 3, nb, width), F32),
            pltpu.VMEM((ITERS, ftiles, 3, nb, width), F32),
            pltpu.VMEM((2, width), F32),
            pltpu.VMEM((nf * nt, 2, width), F32),
            dma((6,)),
            dma((2, count)),
            dma((2,)),
            dma((ITERS, halo)),
            dma((ITERS, halo)),
            dma((ITERS, halo)),
            dma((ITERS, halo)),
            dma((ITERS, ftiles)),
            dma((ITERS, ftiles)),
            dma((ITERS, ftiles)),
            dma((ITERS, ftiles)),
            dma((nf * nt,)),
            dma((nf * nt,)),
        ],
        compiler_params=pltpu.CompilerParams(
            collective_id=0, has_side_effects=True, vmem_limit_bytes=67043328
        ),
    )(vis, model, block_rows, block_cols, flags, prior, couplings, damping.reshape(1, -1))
    return gains, changes[0, :ITERS]


def solution(mesh):
    placed = (
        P("freq", "tm", None, None, None, None),
        P("freq", "tm", None, None, None, None),
        P("freq", "tm", None),
        P("freq", "tm", None),
        P("freq", "tm", None),
        P("freq", "tm", None, None),
        P(),
        P(),
    )
    return jax.shard_map(
        per_device,
        mesh=mesh,
        in_specs=placed,
        out_specs=(P("freq", "tm", None, None), P()),
        check_vma=False,
    )
```
